8 devices in a mesh: dp: 2 (over z, y), tp: 4 (over x, core).
Axes of the slice: x: 2, y: 2, z: 1, core: 2. Of those that a mesh axis runs over, the one named last changes fastest.
Arguments:
- x_in: bfloat16 [2, 128, 5120], P('dp', 'tp'), parts along dimension 0
- ln1_gain: float32 [2, 5120], replicated
- w_qkv: bfloat16 [2, 5120, 40, 384], P(None, None, 'tp')
- w_out: bfloat16 [2, 40, 128, 5120], P(None, 'tp')
- ln2_gain: float32 [2, 5120], replicated
- w_up: bfloat16 [2, 5120, 20480], P(None, None, 'tp')
- w_down: bfloat16 [2, 20480, 5120], P(None, 'tp')
Outputs:
- output: bfloat16 [2, 128, 5120], P('dp', 'tp'), parts along dimension 0
There are 2 independent parts. The reference program is written for one: setup_inputs(seed, part) draws one part's arguments, and reference() takes and returns one part's arrays. A program takes and returns all parts, laid end to end along the dimension named above; an argument that names none is the same for every part.
All inputs are finite; a program needn't handle non-finite values.
Results may differ from the reference program's by a relative error of at most 0.02.
Values are sent between devices in bfloat16 or wider.
A program may use at most 1.25 GiB of HBM per device.

```python
import jax
import jax.numpy as jnp
from jax import lax

D = 5120
HEADS = 40
FF = 20480
LAYERS = 2
BATCH = 1
SEQ = 128
HEAD_DIM = D // HEADS
LN_EPS = 1.0e-5
NEG_BIG = -1.0e30


def setup_inputs(seed: int = 0, part: int = 0) -> dict:
    base_key = jax.random.key(seed)
    key_list = jax.random.split(base_key, 7)
    x_in = jax.random.normal(jax.random.fold_in(key_list[0], part), (BATCH, SEQ, D), jnp.float32)
    ln1_gain = jax.random.uniform(key_list[1], (LAYERS, D), jnp.float32, 1.2, 2.0)
    w_qkv = jax.random.normal(key_list[2], (LAYERS, D, HEADS, 3 * HEAD_DIM), jnp.float32) * D ** -0.5
    w_out = jax.random.normal(key_list[3], (LAYERS, HEADS, HEAD_DIM, D), jnp.float32) * D ** -0.5
    ln2_gain = jax.random.uniform(key_list[4], (LAYERS, D), jnp.float32, 0.7, 1.5)
    w_up = jax.random.normal(key_list[5], (LAYERS, D, FF), jnp.float32) * D ** -0.5
    w_down = jax.random.normal(key_list[6], (LAYERS, FF, D), jnp.float32) * FF ** -0.5
    return {'x_in': x_in.astype(jnp.bfloat16), 'ln1_gain': ln1_gain, 'w_qkv': w_qkv.astype(jnp.bfloat16), 'w_out': w_out.astype(jnp.bfloat16), 'ln2_gain': ln2_gain, 'w_up': w_up.astype(jnp.bfloat16), 'w_down': w_down.astype(jnp.bfloat16)}


def layer_norm(residual, ln_gain):
    resid_f32 = residual.astype(jnp.float32)
    row_mean = jnp.mean(resid_f32, axis=-1, keepdims=True)
    centered = resid_f32 - row_mean
    row_var = jnp.mean(centered * centered, axis=-1, keepdims=True)
    return (centered * lax.rsqrt(row_var + LN_EPS) * ln_gain).astype(jnp.bfloat16)


def attend_head(qkv_head):
    query_blk = qkv_head[:, :HEAD_DIM]
    key_blk = qkv_head[:, HEAD_DIM:2 * HEAD_DIM]
    value_blk = qkv_head[:, 2 * HEAD_DIM:]
    scores = jnp.dot(query_blk, key_blk.T, preferred_element_type=jnp.float32) * HEAD_DIM ** -0.5
    positions = jnp.arange(SEQ)
    scores = jnp.where(positions[:, None] >= positions[None, :], scores, NEG_BIG)
    attn_probs = jax.nn.softmax(scores, axis=-1).astype(jnp.bfloat16)
    return jnp.dot(attn_probs, value_blk, preferred_element_type=jnp.float32).astype(jnp.bfloat16)


def reference(x_in, ln1_gain, w_qkv, w_out, ln2_gain, w_up, w_down):
    def one_layer(residual, layer_weights):
        gain_one, qkv_weight, out_weight, gain_two, up_weight, down_weight = layer_weights
        normed = layer_norm(residual, gain_one)
        qkv_all = jnp.dot(normed, qkv_weight.reshape(D, 3 * D), preferred_element_type=jnp.float32).astype(jnp.bfloat16)
        qkv_heads = qkv_all.reshape(BATCH, SEQ, HEADS, 3 * HEAD_DIM).transpose(0, 2, 1, 3).reshape(BATCH * HEADS, SEQ, 3 * HEAD_DIM)
        attended = lax.map(attend_head, qkv_heads)
        attended = attended.reshape(BATCH, HEADS, SEQ, HEAD_DIM).transpose(0, 2, 1, 3).reshape(BATCH * SEQ, D)
        attn_proj = jnp.dot(attended, out_weight.reshape(D, D), preferred_element_type=jnp.float32)
        residual = (residual.astype(jnp.float32) + attn_proj).astype(jnp.bfloat16)
        normed = layer_norm(residual, gain_two)
        hidden = jax.nn.gelu(jnp.dot(normed, up_weight, preferred_element_type=jnp.float32), approximate=True).astype(jnp.bfloat16)
        down_out = jnp.dot(hidden, down_weight, preferred_element_type=jnp.float32)
        residual = (residual.astype(jnp.float32) + down_out).astype(jnp.bfloat16)
        return residual, None
    resid_out, _ = lax.scan(one_layer, x_in.reshape(BATCH * SEQ, D), (ln1_gain, w_qkv, w_out, ln2_gain, w_up, w_down))
    return resid_out.reshape(BATCH, SEQ, D)
```

```python
import functools

import jax
import jax.numpy as jnp
from jax import lax
from jax.experimental import pallas as pl
from jax.experimental.pallas import tpu as pltpu
from jax.sharding import PartitionSpec as P

LN_EPS = 1.0e-5
NEG_BIG = -1.0e30
MESH = pl.DeviceIdType.MESH

TP = 4
SEQ = 128
ROWS = SEQ // TP
D = 5120
C = 1280
NC = D // C
HEADS = 10
HD = 128
SLOTS = 16
LAYERS = 2
NW = 256


def stack_kernel(x_hbm, g1_ref, wqkv_hbm, wout_hbm, g2_ref, wup_hbm, wdown_hbm, y_hbm,
                 ring, a_all, hid, acc, att, xres, p_snd, p_rcv, q_snd, q_rcv,
                 ring_sem, x_sem, ag_s, ag_r, p_s, p_r, q_s, q_r):
    me = lax.axis_index('tp')
    partner = me + 1 - 2 * lax.rem(me, 2)
    cross = lax.rem(me + 2, TP)
    diag = lax.rem(partner + 2, TP)

    def tile(w, layer, row, col, slot):
        rows = pl.ds(pl.multiple_of(row * C, C), C)
        cols = pl.ds(pl.multiple_of(col * C, C), C)
        return pltpu.make_async_copy(w.at[layer, rows, cols], ring.at[slot], ring_sem.at[slot])

    def start_qkv(layer, i):
        j, s = i // 3, i % 3
        rows = pl.ds(j * C, C)
        pieces, col = [], 0
        for head in range(HEADS):
            lo, hi = head * 3 * HD, (head + 1) * 3 * HD
            a, b = max(lo, s * C), min(hi, (s + 1) * C)
            if a < b:
                pieces.append((head, a - lo, b - a, a - s * C))
        for head, src, width, dst in pieces:
            pltpu.make_async_copy(wqkv_hbm.at[layer, head, rows, pl.ds(src, width)],
                                  ring.at[i, :, pl.ds(dst, width)], ring_sem.at[i]).start(priority=1)

    def start_attention_tile(layer, i):
        if i < 12:
            start_qkv(layer, i)
        else:
            tile(wout_hbm, layer, 0, i - 12, i).start(priority=1)

    def start_up(layer, i):
        tile(wup_hbm, layer, i // NC, lax.rem(i, NC), i).start(priority=1)

    def start_down(layer, i):
        tile(wdown_hbm, layer, lax.rem(i, NC), i // NC, i).start(priority=1)

    def wait_tile(slot):
        tile(wup_hbm, 0, 0, 0, slot).wait()

    def step(lhs, slot, dst, first, finish=None):
        lhs_val = lhs.reshape(SEQ, C)
        for n in range(C // NW):
            cols = pl.ds(n * NW, NW)
            part = jnp.dot(lhs_val, ring[slot, :, cols], preferred_element_type=jnp.float32)
            if not first:
                part = part + acc[dst, :, :, cols].reshape(SEQ, NW)
            if finish is None:
                acc[dst, :, :, cols] = part.reshape(TP, ROWS, NW)
            else:
                finish(part, cols)

    def remote(src, dst, send_sem, recv_sem, peer):
        return pltpu.make_async_remote_copy(src_ref=src, dst_ref=dst, send_sem=send_sem, recv_sem=recv_sem,
                                            device_id={'tp': peer}, device_id_type=MESH)

    def ag_copy(j, kind):
        block, peer = ((me, partner), (me, cross), (cross, partner))[kind]
        return remote(a_all.at[j, block], a_all.at[j, block], ag_s.at[kind, j], ag_r.at[kind, j], peer)

    def ag_wait(j, kind):
        block = (partner, cross, diag)[kind]
        remote(a_all.at[j, block], a_all.at[j, block], ag_s.at[kind, j], ag_r.at[kind, j], partner).wait_recv()

    def norm_and_send(g_ref, layer):
        total = jnp.zeros((ROWS, 1), jnp.float32)
        for j in range(NC):
            total += jnp.sum(xres[j].astype(jnp.float32), axis=-1, keepdims=True)
        mean = total / D
        total = jnp.zeros((ROWS, 1), jnp.float32)
        for j in range(NC):
            centered = xres[j].astype(jnp.float32) - mean
            total += jnp.sum(centered * centered, axis=-1, keepdims=True)
        scale = lax.rsqrt(total / D + LN_EPS)
        for j in range(NC):
            gain = g_ref[pl.ds(layer, 1), pl.ds(j * C, C)]
            a_all[j, me] = ((xres[j].astype(jnp.float32) - mean) * scale * gain).astype(jnp.bfloat16)
            ag_copy(j, 1).start()
            ag_copy(j, 0).start()

    def forward(j):
        ag_wait(j, 1)
        ag_copy(j, 2).start()

    def ag_drain():
        for j in range(NC):
            for kind in range(3):
                ag_copy(j, kind).wait_send()

    def rs_p(q):
        return remote(p_snd.at[q], p_rcv.at[q], p_s.at[q], p_r.at[q], partner)

    def rs_q(q):
        return remote(q_snd.at[q], q_rcv.at[q], q_s.at[q], q_r.at[q], cross)

    def rs_a(q):
        p_snd[q, 0] = acc[q, partner].astype(jnp.bfloat16)
        p_snd[q, 1] = acc[q, diag].astype(jnp.bfloat16)
        rs_p(q).start()

    def rs_b(q):
        rs_p(q).wait_recv()
        q_snd[q] = (acc[q, cross] + p_rcv[q, 1].astype(jnp.float32)).astype(jnp.bfloat16)
        rs_q(q).start()

    def rs_c(q):
        rs_q(q).wait_recv()
        total = acc[q, me] + p_rcv[q, 0].astype(jnp.float32) + q_rcv[q].astype(jnp.float32)
        xres[q] = (xres[q].astype(jnp.float32) + total).astype(jnp.bfloat16)

    def rs_drain():
        for q in range(NC):
            rs_p(q).wait_send()
            rs_q(q).wait_send()

    def attention():
        rows = lax.broadcasted_iota(jnp.int32, (SEQ, SEQ), 0)
        cols = lax.broadcasted_iota(jnp.int32, (SEQ, SEQ), 1)
        causal = rows >= cols

        def part(block):
            third, col = block * HD // C, block * HD % C
            return acc[third, :, :, pl.ds(col, HD)].reshape(SEQ, HD).astype(jnp.bfloat16)

        for head in range(HEADS):
            query, key, value = part(3 * head), part(3 * head + 1), part(3 * head + 2)
            scores = lax.dot_general(query, key, (((1,), (1,)), ((), ())), preferred_element_type=jnp.float32)
            scores = jnp.where(causal, scores * HD ** -0.5, NEG_BIG)
            probs = jnp.exp(scores - jnp.max(scores, axis=-1, keepdims=True))
            probs = (probs / jnp.sum(probs, axis=-1, keepdims=True)).astype(jnp.bfloat16)
            out = jnp.dot(probs, value, preferred_element_type=jnp.float32)
            att[:, pl.ds(head * HD, HD)] = out.astype(jnp.bfloat16)

    x_copies = [pltpu.make_async_copy(x_hbm.at[0, :, pl.ds(j * C, C)], xres.at[j], x_sem) for j in range(NC)]
    for copy in x_copies:
        copy.start()
    for i in range(SLOTS):
        start_attention_tile(0, i)
    barrier = pltpu.get_barrier_semaphore()
    for peer in (partner, cross):
        pl.semaphore_signal(barrier, inc=1, device_id={'tp': peer}, device_id_type=MESH)
    pl.semaphore_wait(barrier, 2)
    for copy in x_copies:
        copy.wait()

    def loop(lo, hi, body):
        lax.fori_loop(lo, hi, lambda i, carry: (body(i), carry)[1], 0)

    def layer_body(layer):
        norm_and_send(g1_ref, layer)
        forward(0)

        def qkv_chunk(j, first):
            ag_wait(j, 0)
            ag_wait(j, 2)

            def third(s):
                i = 3 * j + s
                wait_tile(i)
                step(a_all[j], i, s, first)
                start_up(layer, i)

            third(0)

            @pl.when(j < NC - 1)
            def _():
                forward(j + 1)

            loop(1, 3, third)

        qkv_chunk(0, True)
        loop(1, NC, lambda j: qkv_chunk(j, False))
        ag_drain()
        attention()

        def out_quarter(q):
            wait_tile(12 + q)
            step(att[...], 12 + q, q, True)
            start_up(layer, 12 + q)
            rs_a(q)

            @pl.when(q >= 2)
            def _():
                rs_b(q - 2)

        loop(0, NC, out_quarter)
        rs_b(2)
        rs_b(3)
        loop(0, NC, rs_c)
        rs_drain()

        norm_and_send(g2_ref, layer)
        forward(0)

        def up_chunk(j, first, last):
            ag_wait(j, 0)
            ag_wait(j, 2)

            def quarter(q):
                i = NC * j + q

                def finish(part, cols):
                    hid[q, :, cols] = jax.nn.gelu(part, approximate=True).astype(jnp.bfloat16)

                wait_tile(i)
                step(a_all[j], i, q, first, finish if last else None)
                start_down(layer, i)

            quarter(0)
            if not last:
                forward(j + 1)
            loop(1, NC, quarter)

        up_chunk(0, True, False)
        loop(1, NC - 1, lambda j: up_chunk(j, False, False))
        up_chunk(NC - 1, False, True)
        ag_drain()

        def next_tiles(i):
            @pl.when(layer < LAYERS - 1)
            def _():
                for k in range(SLOTS):
                    @pl.when(i == k)
                    def _():
                        start_attention_tile(layer + 1, k)

        def down_quarter(q):
            def chunk(j, first):
                i = NC * q + j
                wait_tile(i)
                step(hid[j], i, q, first)
                next_tiles(i)

            chunk(0, True)
            chunk(1, False)

            @pl.when(q >= 1)
            def _():
                rs_b(q - 1)

            loop(2, NC, lambda j: chunk(j, False))
            rs_a(q)

        loop(0, NC, down_quarter)
        rs_b(NC - 1)
        loop(0, NC, rs_c)
        rs_drain()

    loop(0, LAYERS, layer_body)
    y_copies = [pltpu.make_async_copy(xres.at[j], y_hbm.at[0, :, pl.ds(j * C, C)], x_sem) for j in range(NC)]
    for copy in y_copies:
        copy.start()
    for copy in y_copies:
        copy.wait()


def solution(mesh):
    def layer_stack(x_local, ln1_gain, w_qkv, w_out, ln2_gain, w_up, w_down):
        w_qkv = jnp.transpose(w_qkv, (0, 2, 1, 3))
        w_out = w_out.reshape(LAYERS, HEADS * HD, D)
        hbm = pl.BlockSpec(memory_space=pl.ANY)
        vmem = pl.BlockSpec(memory_space=pltpu.VMEM)
        weight_bytes = 2 * LAYERS * (3 * C * D + C * D + 2 * D * D)
        return pl.pallas_call(
            stack_kernel,
            out_shape=jax.ShapeDtypeStruct(x_local.shape, jnp.bfloat16),
            in_specs=[hbm, vmem, hbm, hbm, vmem, hbm, hbm],
            out_specs=hbm,
            scratch_shapes=[
                pltpu.VMEM((SLOTS, C, C), jnp.bfloat16),
                pltpu.VMEM((NC, TP, ROWS, C), jnp.bfloat16),
                pltpu.VMEM((NC, SEQ, C), jnp.bfloat16),
                pltpu.VMEM((NC, TP, ROWS, C), jnp.float32),
                pltpu.VMEM((SEQ, C), jnp.bfloat16),
                pltpu.VMEM((NC, ROWS, C), jnp.bfloat16),
                pltpu.VMEM((NC, 2, ROWS, C), jnp.bfloat16),
                pltpu.VMEM((NC, 2, ROWS, C), jnp.bfloat16),
                pltpu.VMEM((NC, ROWS, C), jnp.bfloat16),
                pltpu.VMEM((NC, ROWS, C), jnp.bfloat16),
                pltpu.SemaphoreType.DMA((SLOTS,)),
                pltpu.SemaphoreType.DMA,
                pltpu.SemaphoreType.DMA((3, NC)),
                pltpu.SemaphoreType.DMA((3, NC)),
                pltpu.SemaphoreType.DMA((NC,)),
                pltpu.SemaphoreType.DMA((NC,)),
                pltpu.SemaphoreType.DMA((NC,)),
                pltpu.SemaphoreType.DMA((NC,)),
            ],
            compiler_params=pltpu.CompilerParams(collective_id=0, has_side_effects=True, vmem_limit_bytes=67_043_328),
            cost_estimate=pl.CostEstimate(flops=SEQ * weight_bytes, bytes_accessed=weight_bytes, transcendentals=0),
        )(x_local, ln1_gain, w_qkv, w_out, ln2_gain, w_up, w_down)

    return jax.shard_map(layer_stack, mesh=mesh, in_specs=(P('dp', 'tp', None), P(), P(None, None, 'tp', None), P(None, 'tp', None, None), P(), P(None, None, 'tp'), P(None, 'tp', None)), out_specs=P('dp', 'tp', None), check_vma=False)
```

```python
import functools

import jax
import jax.numpy as jnp
from jax import lax
from jax.experimental import pallas as pl
from jax.experimental.pallas import tpu as pltpu
from jax.sharding import PartitionSpec as P

LN_EPS = 1.0e-5
NEG_BIG = -1.0e30
MESH = pl.DeviceIdType.MESH

TP = 4
SEQ = 128
ROWS = SEQ // TP
D = 5120
C = 1280
NC = D // C
HEADS = 10
HD = 128
SLOTS = 16
LAYERS = 2
NW = 256


def stack_kernel(x_hbm, g1_hbm, wqkv_hbm, wout_hbm, g2_hbm, wup_hbm, wdown_hbm, y_hbm,
                 ring, a_all, hid, acc, att, s_buf, p_buf, xres, p_snd, p_rcv, q_snd, q_rcv, g1_ref, g2_ref,
                 ring_sem, x_sem, g_sem, ag_s, ag_r, p_s, p_r, q_s, q_r):
    me = lax.axis_index('tp')
    partner = me + 1 - 2 * lax.rem(me, 2)
    cross = lax.rem(me + 2, TP)
    diag = lax.rem(partner + 2, TP)

    def tile(w, layer, row, col, slot):
        rows = pl.ds(pl.multiple_of(row * C, C), C)
        cols = pl.ds(pl.multiple_of(col * C, C), C)
        return pltpu.make_async_copy(w.at[layer, rows, cols], ring.at[slot], ring_sem.at[slot])

    def start_qkv(layer, i):
        j, s = i // 3, i % 3
        rows = pl.ds(j * C, C)
        pieces, col = [], 0
        for head in range(HEADS):
            lo, hi = head * 3 * HD, (head + 1) * 3 * HD
            a, b = max(lo, s * C), min(hi, (s + 1) * C)
            if a < b:
                pieces.append((head, a - lo, b - a, a - s * C))
        for head, src, width, dst in pieces:
            pltpu.make_async_copy(wqkv_hbm.at[layer, head, rows, pl.ds(src, width)],
                                  ring.at[i, :, pl.ds(dst, width)], ring_sem.at[i]).start(priority=1)

    def start_attention_tile(layer, i):
        if i < 12:
            start_qkv(layer, i)
        else:
            tile(wout_hbm, layer, 0, i - 12, i).start(priority=1)

    def start_up(layer, i):
        tile(wup_hbm, layer, i // NC, lax.rem(i, NC), i).start(priority=1)

    def start_down(layer, i):
        tile(wdown_hbm, layer, lax.rem(i, NC), i // NC, i).start(priority=1)

    def wait_tile(slot):
        tile(wup_hbm, 0, 0, 0, slot).wait()

    def block(jobs):
        for pairs, dst, add, finish in jobs:
            for n in range(C // NW):
                cols = pl.ds(n * NW, NW)
                part = None
                for lhs, slot in pairs:
                    term = jnp.dot(lhs(), ring[slot, :, cols], preferred_element_type=jnp.float32)
                    part = term if part is None else part + term
                if add:
                    part = part + acc[dst, :, :, cols].reshape(SEQ, NW)
                if finish is None:
                    acc[dst, :, :, cols] = part.reshape(TP, ROWS, NW)
                else:
                    finish(part, dst, cols)

    def remote(src, dst, send_sem, recv_sem, peer):
        return pltpu.make_async_remote_copy(src_ref=src, dst_ref=dst, send_sem=send_sem, recv_sem=recv_sem,
                                            device_id={'tp': peer}, device_id_type=MESH)

    def ag_copy(j, kind):
        block, peer = ((me, partner), (me, cross), (cross, partner))[kind]
        return remote(a_all.at[j, block], a_all.at[j, block], ag_s.at[kind, j], ag_r.at[kind, j], peer)

    def ag_wait(j, kind):
        block = (partner, cross, diag)[kind]
        remote(a_all.at[j, block], a_all.at[j, block], ag_s.at[kind, j], ag_r.at[kind, j], partner).wait_recv()

    def norm_and_send(g_ref, layer):
        total = jnp.zeros((ROWS, 1), jnp.float32)
        for j in range(NC):
            total += jnp.sum(xres[j].astype(jnp.float32), axis=-1, keepdims=True)
        mean = total / D
        total = jnp.zeros((ROWS, 1), jnp.float32)
        for j in range(NC):
            centered = xres[j].astype(jnp.float32) - mean
            total += jnp.sum(centered * centered, axis=-1, keepdims=True)
        scale = lax.rsqrt(total / D + LN_EPS)
        for j in range(NC):
            gain = g_ref[pl.ds(layer, 1), pl.ds(j * C, C)]
            a_all[j, me] = ((xres[j].astype(jnp.float32) - mean) * scale * gain).astype(jnp.bfloat16)
            ag_copy(j, 1).start()
            ag_copy(j, 0).start()

    def forward(j):
        ag_wait(j, 1)
        ag_copy(j, 2).start()

    def ag_drain():
        for j in range(NC):
            for kind in range(3):
                ag_copy(j, kind).wait_send()

    def rs_p(q):
        return remote(p_snd.at[q], p_rcv.at[q], p_s.at[q], p_r.at[q], partner)

    def rs_q(q):
        return remote(q_snd.at[q], q_rcv.at[q], q_s.at[q], q_r.at[q], cross)

    def rs_a(q):
        p_snd[q, 0] = acc[q, partner].astype(jnp.bfloat16)
        p_snd[q, 1] = acc[q, diag].astype(jnp.bfloat16)
        rs_p(q).start()

    def rs_b(q):
        rs_p(q).wait_recv()
        q_snd[q] = (acc[q, cross] + p_rcv[q, 1].astype(jnp.float32)).astype(jnp.bfloat16)
        rs_q(q).start()

    def rs_c(q):
        rs_q(q).wait_recv()
        total = acc[q, me] + p_rcv[q, 0].astype(jnp.float32) + q_rcv[q].astype(jnp.float32)
        xres[q] = (xres[q].astype(jnp.float32) + total).astype(jnp.bfloat16)

    def rs_drain():
        for q in range(NC):
            rs_p(q).wait_send()
            rs_q(q).wait_send()

    def attention():
        keys = lax.broadcasted_iota(jnp.int32, (SEQ, SEQ), 0)
        queries = lax.broadcasted_iota(jnp.int32, (SEQ, SEQ), 1)
        causal = queries >= keys

        def part(block):
            third, col = block * HD // C, block * HD % C
            return acc[third, :, :, pl.ds(col, HD)].reshape(SEQ, HD).astype(jnp.bfloat16)

        for head in range(HEADS):
            query, key = part(3 * head), part(3 * head + 1)
            scores = lax.dot_general(key, query, (((1,), (1,)), ((), ())), preferred_element_type=jnp.float32)
            s_buf[head] = jnp.where(causal, scores * HD ** -0.5, NEG_BIG)
        for head in range(HEADS):
            scores = s_buf[head]
            probs = jnp.exp(scores - jnp.max(scores, axis=0, keepdims=True))
            p_buf[head] = (probs / jnp.sum(probs, axis=0, keepdims=True)).astype(jnp.bfloat16)
        for head in range(HEADS):
            out = lax.dot_general(p_buf[head], part(3 * head + 2), (((0,), (0,)), ((), ())),
                                  preferred_element_type=jnp.float32)
            att[:, pl.ds(head * HD, HD)] = out.astype(jnp.bfloat16)

    x_copies = [pltpu.make_async_copy(x_hbm.at[0, :, pl.ds(j * C, C)], xres.at[j], x_sem.at[j]) for j in range(NC)]
    g_copies = [pltpu.make_async_copy(g1_hbm, g1_ref, g_sem.at[0]), pltpu.make_async_copy(g2_hbm, g2_ref, g_sem.at[1])]
    for copy in x_copies + g_copies:
        copy.start()
    for i in range(SLOTS):
        start_attention_tile(0, i)
    barrier = pltpu.get_barrier_semaphore()
    for peer in (partner, cross):
        pl.semaphore_signal(barrier, inc=1, device_id={'tp': peer}, device_id_type=MESH)
    pl.semaphore_wait(barrier, 2)
    for copy in x_copies + g_copies:
        copy.wait()

    def loop(lo, hi, body):
        lax.fori_loop(lo, hi, lambda i, carry: (body(i), carry)[1], 0)

    def layer_body(layer):
        norm_and_send(g1_ref, layer)
        forward(0)

        def qkv_tiles(j, thirds, first):
            for t in thirds:
                wait_tile(3 * j + t)
            block([([(lambda: a_all[j].reshape(SEQ, C), 3 * j + t)], t, not first, None) for t in thirds])
            for t in thirds:
                start_up(layer, 3 * j + t)

        def qkv_chunk(j, first, last):
            ag_wait(j, 0)
            ag_wait(j, 2)
            if last:
                qkv_tiles(j, (0, 1, 2), first)
            else:
                qkv_tiles(j, (0,), first)
                forward(j + 1)
                qkv_tiles(j, (1, 2), first)

        qkv_chunk(0, True, False)
        loop(1, NC - 1, lambda j: qkv_chunk(j, False, False))
        qkv_chunk(NC - 1, False, True)
        ag_drain()
        attention()

        def out_tiles(quarters):
            for q in quarters:
                wait_tile(12 + q)
            block([([(lambda: att[...], 12 + q)], q, False, None) for q in quarters])
            for q in quarters:
                rs_a(q)
            for q in quarters:
                start_up(layer, 12 + q)

        out_tiles((0, 1))
        out_tiles((2, 3))
        loop(0, NC, rs_b)
        loop(0, NC, rs_c)
        rs_drain()

        norm_and_send(g2_ref, layer)
        forward(0)

        def gelu_out(part, q, cols):
            hid[q, :, cols] = jax.nn.gelu(part, approximate=True).astype(jnp.bfloat16)

        def up_tiles(j, quarters, first, last):
            for q in quarters:
                wait_tile(NC * j + q)
            block([([(lambda: a_all[j].reshape(SEQ, C), NC * j + q)], q, not first, gelu_out if last else None)
                   for q in quarters])
            for q in quarters:
                start_down(layer, NC * j + q)

        def up_chunk(j, first, last):
            ag_wait(j, 0)
            ag_wait(j, 2)
            if last:
                up_tiles(j, (0, 1, 2, 3), first, last)
            else:
                up_tiles(j, (0, 1), first, last)
                forward(j + 1)
                up_tiles(j, (2, 3), first, last)

        up_chunk(0, True, False)
        loop(1, NC - 1, lambda j: up_chunk(j, False, False))
        up_chunk(NC - 1, False, True)
        ag_drain()

        def next_tiles(q, chunks):
            @pl.when(layer < LAYERS - 1)
            def _():
                if isinstance(q, int):
                    for j in chunks:
                        start_attention_tile(layer + 1, NC * q + j)
                else:
                    for k in range(NC - 1):
                        @pl.when(q == k)
                        def _():
                            for j in chunks:
                                start_attention_tile(layer + 1, NC * k + j)

        def down_tiles(q, chunks, add):
            for j in chunks:
                wait_tile(NC * q + j)
            block([([(functools.partial(lambda j: hid[j], j), NC * q + j) for j in chunks], q, add, None)])

        def down_quarter(q):
            down_tiles(q, (0, 1, 2, 3), False)
            rs_a(q)
            next_tiles(q, (0, 1, 2, 3))

            @pl.when(q >= 1)
            def _():
                rs_b(q - 1)

        loop(0, NC - 1, down_quarter)
        last = NC - 1
        down_tiles(last, (0, 1), False)
        rs_b(last - 1)
        next_tiles(last, (0, 1))
        down_tiles(last, (2, 3), True)
        rs_a(last)
        next_tiles(last, (2, 3))
        rs_b(last)
        loop(0, NC, rs_c)
        rs_drain()

    loop(0, LAYERS, layer_body)
    y_copies = [pltpu.make_async_copy(xres.at[j], y_hbm.at[0, :, pl.ds(j * C, C)], x_sem.at[j]) for j in range(NC)]
    for copy in y_copies:
        copy.start()
    for copy in y_copies:
        copy.wait()


def solution(mesh):
    def layer_stack(x_local, ln1_gain, w_qkv, w_out, ln2_gain, w_up, w_down):
        w_qkv = jnp.transpose(w_qkv, (0, 2, 1, 3))
        w_out = w_out.reshape(LAYERS, HEADS * HD, D)
        hbm = pl.BlockSpec(memory_space=pl.ANY)
        weight_bytes = 2 * LAYERS * (3 * C * D + C * D + 2 * D * D)
        return pl.pallas_call(
            stack_kernel,
            out_shape=jax.ShapeDtypeStruct(x_local.shape, jnp.bfloat16),
            in_specs=[hbm] * 7,
            out_specs=hbm,
            scratch_shapes=[
                pltpu.VMEM((SLOTS, C, C), jnp.bfloat16),
                pltpu.VMEM((NC, TP, ROWS, C), jnp.bfloat16),
                pltpu.VMEM((NC, SEQ, C), jnp.bfloat16),
                pltpu.VMEM((NC, TP, ROWS, C), jnp.float32),
                pltpu.VMEM((SEQ, C), jnp.bfloat16),
                pltpu.VMEM((HEADS, SEQ, SEQ), jnp.float32),
                pltpu.VMEM((HEADS, SEQ, SEQ), jnp.bfloat16),
                pltpu.VMEM((NC, ROWS, C), jnp.bfloat16),
                pltpu.VMEM((NC, 2, ROWS, C), jnp.bfloat16),
                pltpu.VMEM((NC, 2, ROWS, C), jnp.bfloat16),
                pltpu.VMEM((NC, ROWS, C), jnp.bfloat16),
                pltpu.VMEM((NC, ROWS, C), jnp.bfloat16),
                pltpu.VMEM((LAYERS, D), jnp.float32),
                pltpu.VMEM((LAYERS, D), jnp.float32),
                pltpu.SemaphoreType.DMA((SLOTS,)),
                pltpu.SemaphoreType.DMA((NC,)),
                pltpu.SemaphoreType.DMA((2,)),
                pltpu.SemaphoreType.DMA((3, NC)),
                pltpu.SemaphoreType.DMA((3, NC)),
                pltpu.SemaphoreType.DMA((NC,)),
                pltpu.SemaphoreType.DMA((NC,)),
                pltpu.SemaphoreType.DMA((NC,)),
                pltpu.SemaphoreType.DMA((NC,)),
            ],
            compiler_params=pltpu.CompilerParams(collective_id=0, has_side_effects=True, vmem_limit_bytes=67_043_328),
            cost_estimate=pl.CostEstimate(flops=SEQ * weight_bytes, bytes_accessed=weight_bytes, transcendentals=0),
        )(x_local, ln1_gain, w_qkv, w_out, ln2_gain, w_up, w_down)

    return jax.shard_map(layer_stack, mesh=mesh, in_specs=(P('dp', 'tp', None), P(), P(None, None, 'tp', None), P(None, 'tp', None, None), P(), P(None, None, 'tp'), P(None, 'tp', None)), out_specs=P('dp', 'tp', None), check_vma=False)
```

```python
import functools

import jax
import jax.numpy as jnp
from jax import lax
from jax.experimental import pallas as pl
from jax.experimental.pallas import tpu as pltpu
from jax.sharding import PartitionSpec as P

LN_EPS = 1.0e-5
NEG_BIG = -1.0e30
MESH = pl.DeviceIdType.MESH

TP = 4
SEQ = 128
ROWS = SEQ // TP
D = 5120
C = 1280
NC = D // C
HEADS = 10
HD = 128
SLOTS = 16
LAYERS = 2
NW = 256


def stack_kernel(x_hbm, g1_hbm, wqkv_hbm, wout_hbm, g2_hbm, wup_hbm, wdown_hbm, y_hbm,
                 ring, x_all, a_buf, stat, q_stat, mean_b, scale_b, hid, acc, att, s_buf, p_buf, p_snd, p_rcv, q_snd, q_rcv, g1_ref, g2_ref,
                 ring_sem, x_sem, g_sem, ag_s, ag_r, st_s, st_r, p_s, p_r, q_s, q_r):
    me = lax.axis_index('tp')
    partner = me + 1 - 2 * lax.rem(me, 2)
    cross = lax.rem(me + 2, TP)
    diag = lax.rem(partner + 2, TP)

    def tile(w, layer, row, col, slot):
        rows = pl.ds(pl.multiple_of(row * C, C), C)
        cols = pl.ds(pl.multiple_of(col * C, C), C)
        return pltpu.make_async_copy(w.at[layer, rows, cols], ring.at[slot], ring_sem.at[slot])

    def start_qkv(layer, i):
        j, s = i // 3, i % 3
        rows = pl.ds(j * C, C)
        pieces, col = [], 0
        for head in range(HEADS):
            lo, hi = head * 3 * HD, (head + 1) * 3 * HD
            a, b = max(lo, s * C), min(hi, (s + 1) * C)
            if a < b:
                pieces.append((head, a - lo, b - a, a - s * C))
        for head, src, width, dst in pieces:
            pltpu.make_async_copy(wqkv_hbm.at[layer, head, rows, pl.ds(src, width)],
                                  ring.at[i, :, pl.ds(dst, width)], ring_sem.at[i]).start(priority=1)

    def start_attention_tile(layer, i):
        if i < 12:
            start_qkv(layer, i)
        else:
            tile(wout_hbm, layer, 0, i - 12, i).start(priority=1)

    def start_up(layer, i):
        tile(wup_hbm, layer, i // NC, lax.rem(i, NC), i).start(priority=1)

    def start_down(layer, i):
        tile(wdown_hbm, layer, lax.rem(i, NC), i // NC, i).start(priority=1)

    def wait_tile(slot):
        tile(wup_hbm, 0, 0, 0, slot).wait()

    def block(jobs):
        for pairs, dst, add, finish in jobs:
            for n in range(C // NW):
                cols = pl.ds(n * NW, NW)
                part = None
                for lhs, slot in pairs:
                    term = jnp.dot(lhs(), ring[slot, :, cols], preferred_element_type=jnp.float32)
                    part = term if part is None else part + term
                if add:
                    part = part + acc[dst, :, :, cols].reshape(SEQ, NW)
                if finish is None:
                    acc[dst, :, :, cols] = part.reshape(TP, ROWS, NW)
                else:
                    finish(part, dst, cols)

    def remote(src, dst, send_sem, recv_sem, peer):
        return pltpu.make_async_remote_copy(src_ref=src, dst_ref=dst, send_sem=send_sem, recv_sem=recv_sem,
                                            device_id={'tp': peer}, device_id_type=MESH)

    def ag_copy(j, kind):
        source, peer = ((me, partner), (me, cross), (cross, partner))[kind]
        return remote(x_all.at[j, source], x_all.at[j, source], ag_s.at[kind, j], ag_r.at[kind, j], peer)

    def ag_wait(j, kind):
        source = (partner, cross, diag)[kind]
        remote(x_all.at[j, source], x_all.at[j, source], ag_s.at[kind, j], ag_r.at[kind, j], partner).wait_recv()

    def ag_send(j):
        ag_copy(j, 1).start()
        ag_copy(j, 0).start()

    def forward(j):
        ag_wait(j, 1)
        ag_copy(j, 2).start()

    def stat_copy(k):
        return remote(stat.at[me], stat.at[me], st_s.at[k], st_r.at[k], (partner, cross, diag)[k])

    def quarter_stats(j):
        x = x_all[j, me].astype(jnp.float32)
        mean = jnp.sum(x, axis=-1, keepdims=True) / C
        centered = x - mean
        q_stat[j, 0] = jnp.broadcast_to(mean, (ROWS, HD))
        q_stat[j, 1] = jnp.broadcast_to(jnp.sum(centered * centered, axis=-1, keepdims=True), (ROWS, HD))

    def stats_send():
        mean = (q_stat[0, 0] + q_stat[1, 0] + q_stat[2, 0] + q_stat[3, 0]) / NC
        square = jnp.zeros((ROWS, HD), jnp.float32)
        for j in range(NC):
            shift = q_stat[j, 0] - mean
            square += q_stat[j, 1] + C * (shift * shift)
        scale = lax.rsqrt(square / D + LN_EPS)
        lanes = lax.broadcasted_iota(jnp.int32, (8, HD), 1)
        packed = jnp.zeros((8, HD), jnp.float32)
        for i in range(ROWS // 8):
            packed = jnp.where(lanes == i, mean[8 * i:8 * i + 8], packed)
            packed = jnp.where(lanes == 4 + i, scale[8 * i:8 * i + 8], packed)
        stat[me] = packed
        for k in (1, 2, 0):
            stat_copy(k).start()

    def stats_wait():
        for k, source in enumerate((partner, cross, diag)):
            remote(stat.at[source], stat.at[source], st_s.at[k], st_r.at[k], partner).wait_recv()
        for source in range(TP):
            packed = stat[source]
            for i in range(ROWS // 8):
                rows = pl.ds(source * ROWS + 8 * i, 8)
                mean_b[rows] = jnp.broadcast_to(packed[:, i:i + 1], (8, HD))
                scale_b[rows] = jnp.broadcast_to(packed[:, 4 + i:5 + i], (8, HD))

    def ag_drain():
        for j in range(NC):
            for kind in range(3):
                ag_copy(j, kind).wait_send()
        for k in range(3):
            stat_copy(k).wait_send()

    def normalize(j, g_ref, layer):
        mean, scale = mean_b[...], scale_b[...]
        for k in range(C // HD):
            cols = pl.ds(k * HD, HD)
            gains = g_ref[:, pl.ds(pl.multiple_of(j * C + k * HD, HD), HD)]
            gain = jnp.where(layer == 0, gains[0:1], gains[1:2])
            x = x_all[j, :, :, cols].reshape(SEQ, HD).astype(jnp.float32)
            a_buf[:, cols] = ((x - mean) * scale * gain).astype(jnp.bfloat16)

    def rs_p(q):
        return remote(p_snd.at[q], p_rcv.at[q], p_s.at[q], p_r.at[q], partner)

    def rs_q(q):
        return remote(q_snd.at[q], q_rcv.at[q], q_s.at[q], q_r.at[q], cross)

    def rs_a(q):
        p_snd[q, 0] = acc[q, partner].astype(jnp.bfloat16)
        p_snd[q, 1] = acc[q, diag].astype(jnp.bfloat16)
        rs_p(q).start()

    def rs_b(q):
        rs_p(q).wait_recv()
        q_snd[q] = (acc[q, cross] + p_rcv[q, 1].astype(jnp.float32)).astype(jnp.bfloat16)
        rs_q(q).start()

    def rs_c(q):
        rs_q(q).wait_recv()
        total = acc[q, me] + p_rcv[q, 0].astype(jnp.float32) + q_rcv[q].astype(jnp.float32)
        x_all[q, me] = (x_all[q, me].astype(jnp.float32) + total).astype(jnp.bfloat16)
        quarter_stats(q)

    def rs_drain():
        for q in range(NC):
            rs_p(q).wait_send()
            rs_q(q).wait_send()

    def attention():
        keys = lax.broadcasted_iota(jnp.int32, (SEQ, SEQ), 0)
        queries = lax.broadcasted_iota(jnp.int32, (SEQ, SEQ), 1)
        causal = queries >= keys

        def part(block):
            third, col = block * HD // C, block * HD % C
            return acc[third, :, :, pl.ds(col, HD)].reshape(SEQ, HD).astype(jnp.bfloat16)

        for head in range(HEADS):
            query, key = part(3 * head), part(3 * head + 1)
            scores = lax.dot_general(key, query, (((1,), (1,)), ((), ())), preferred_element_type=jnp.float32)
            s_buf[head] = jnp.where(causal, scores * HD ** -0.5, NEG_BIG)
        for head in range(HEADS):
            scores = s_buf[head]
            probs = jnp.exp(scores - jnp.max(scores, axis=0, keepdims=True))
            p_buf[head] = (probs / jnp.sum(probs, axis=0, keepdims=True)).astype(jnp.bfloat16)
        for head in range(HEADS):
            out = lax.dot_general(p_buf[head], part(3 * head + 2), (((0,), (0,)), ((), ())),
                                  preferred_element_type=jnp.float32)
            att[:, pl.ds(head * HD, HD)] = out.astype(jnp.bfloat16)

    x_copies = [pltpu.make_async_copy(x_hbm.at[0, :, pl.ds(j * C, C)], x_all.at[j, me], x_sem.at[j]) for j in range(NC)]
    g_copies = [pltpu.make_async_copy(g1_hbm, g1_ref, g_sem.at[0]), pltpu.make_async_copy(g2_hbm, g2_ref, g_sem.at[1])]
    for copy in x_copies + g_copies:
        copy.start()
    for i in range(SLOTS):
        start_attention_tile(0, i)
    barrier = pltpu.get_barrier_semaphore()
    for peer in (partner, cross, diag):
        pl.semaphore_signal(barrier, inc=1, device_id={'tp': peer}, device_id_type=MESH)
    pl.semaphore_wait(barrier, 3)
    for copy in x_copies + g_copies:
        copy.wait()

    def loop(lo, hi, body):
        lax.fori_loop(lo, hi, lambda i, carry: (body(i), carry)[1], 0)

    def chunks(chunk):
        stats_wait()

        def one(j, first, last):
            ag_wait(j, 0)
            ag_wait(j, 2)
            chunk(j, first, last)

        one(0, True, False)
        forward(2)

        def middle(j):
            one(j, False, False)

            @pl.when(j == 1)
            def _():
                forward(3)

        loop(1, NC - 1, middle)
        one(NC - 1, False, True)
        ag_drain()

    def layer_body(layer):
        more = layer < LAYERS - 1

        def qkv_chunk(j, first, last):
            for t in range(3):
                wait_tile(3 * j + t)
            normalize(j, g1_ref, layer)
            block([([(lambda: a_buf[...], 3 * j + t)], t, not first, None) for t in range(3)])
            for t in range(3):
                start_up(layer, 3 * j + t)

        chunks(qkv_chunk)
        attention()

        def out_tiles(quarters):
            for q in quarters:
                wait_tile(12 + q)
            block([([(lambda: att[...], 12 + q)], q, False, None) for q in quarters])
            for q in quarters:
                rs_a(q)
            for q in quarters:
                start_up(layer, 12 + q)

        out_tiles((0,))
        out_tiles((1, 2))
        rs_b(0)
        out_tiles((3,))
        loop(1, NC, rs_b)
        for q in range(NC):
            rs_c(q)
            if q < 2:
                ag_send(q)
        stats_send()
        ag_send(2)
        ag_send(3)
        forward(0)
        forward(1)
        rs_drain()

        def gelu_out(part, q, cols):
            hid[q, :, cols] = jax.nn.gelu(part, approximate=True).astype(jnp.bfloat16)

        def up_chunk(j, first, last):
            for q in range(NC):
                wait_tile(NC * j + q)
            normalize(j, g2_ref, layer)
            block([([(lambda: a_buf[...], NC * j + q)], q, not first, gelu_out if last else None) for q in range(NC)])
            for q in range(NC):
                start_down(layer, NC * j + q)

        chunks(up_chunk)

        def down_tiles(q, chunk_ids, add):
            for j in chunk_ids:
                wait_tile(NC * q + j)
            block([([(functools.partial(lambda j: hid[j], j), NC * q + j) for j in chunk_ids], q, add, None)])

            for k in range(NC):
                @pl.when(jnp.logical_and(more, q == k))
                def _():
                    for j in chunk_ids:
                        start_attention_tile(layer + 1, NC * k + j)

        def down_quarter(q):
            down_tiles(q, (0, 1), False)

            @pl.when(q >= 1)
            def _():
                rs_b(q - 1)

            @pl.when(q >= 2)
            def _():
                rs_c(q - 2)

                @pl.when(more)
                def _():
                    ag_send(q - 2)

            down_tiles(q, (2, 3), True)
            rs_a(q)

        loop(0, NC, down_quarter)
        rs_b(3)
        rs_c(2)

        @pl.when(more)
        def _():
            ag_send(2)
            forward(0)
            forward(1)

        rs_c(3)

        @pl.when(more)
        def _():
            stats_send()
            ag_send(3)

        rs_drain()

    ag_send(0)
    for j in range(NC):
        quarter_stats(j)
    stats_send()
    for j in range(1, NC):
        ag_send(j)
    forward(0)
    forward(1)
    loop(0, LAYERS, layer_body)
    y_copies = [pltpu.make_async_copy(x_all.at[j, me], y_hbm.at[0, :, pl.ds(j * C, C)], x_sem.at[j]) for j in range(NC)]
    for copy in y_copies:
        copy.start()
    for copy in y_copies:
        copy.wait()


def solution(mesh):
    def layer_stack(x_local, ln1_gain, w_qkv, w_out, ln2_gain, w_up, w_down):
        w_qkv = jnp.transpose(w_qkv, (0, 2, 1, 3))
        w_out = w_out.reshape(LAYERS, HEADS * HD, D)
        hbm = pl.BlockSpec(memory_space=pl.ANY)
        weight_bytes = 2 * LAYERS * (3 * C * D + C * D + 2 * D * D)
        return pl.pallas_call(
            stack_kernel,
            out_shape=jax.ShapeDtypeStruct(x_local.shape, jnp.bfloat16),
            in_specs=[hbm] * 7,
            out_specs=hbm,
            scratch_shapes=[
                pltpu.VMEM((SLOTS, C, C), jnp.bfloat16),
                pltpu.VMEM((NC, TP, ROWS, C), jnp.bfloat16),
                pltpu.VMEM((SEQ, C), jnp.bfloat16),
                pltpu.VMEM((TP, 8, HD), jnp.float32),
                pltpu.VMEM((NC, 2, ROWS, HD), jnp.float32),
                pltpu.VMEM((SEQ, HD), jnp.float32),
                pltpu.VMEM((SEQ, HD), jnp.float32),
                pltpu.VMEM((NC, SEQ, C), jnp.bfloat16),
                pltpu.VMEM((NC, TP, ROWS, C), jnp.float32),
                pltpu.VMEM((SEQ, C), jnp.bfloat16),
                pltpu.VMEM((HEADS, SEQ, SEQ), jnp.float32),
                pltpu.VMEM((HEADS, SEQ, SEQ), jnp.bfloat16),
                pltpu.VMEM((NC, 2, ROWS, C), jnp.bfloat16),
                pltpu.VMEM((NC, 2, ROWS, C), jnp.bfloat16),
                pltpu.VMEM((NC, ROWS, C), jnp.bfloat16),
                pltpu.VMEM((NC, ROWS, C), jnp.bfloat16),
                pltpu.VMEM((LAYERS, D), jnp.float32),
                pltpu.VMEM((LAYERS, D), jnp.float32),
                pltpu.SemaphoreType.DMA((SLOTS,)),
                pltpu.SemaphoreType.DMA((NC,)),
                pltpu.SemaphoreType.DMA((2,)),
                pltpu.SemaphoreType.DMA((3, NC)),
                pltpu.SemaphoreType.DMA((3, NC)),
                pltpu.SemaphoreType.DMA((3,)),
                pltpu.SemaphoreType.DMA((3,)),
                pltpu.SemaphoreType.DMA((NC,)),
                pltpu.SemaphoreType.DMA((NC,)),
                pltpu.SemaphoreType.DMA((NC,)),
                pltpu.SemaphoreType.DMA((NC,)),
            ],
            compiler_params=pltpu.CompilerParams(collective_id=0, has_side_effects=True, vmem_limit_bytes=67_043_328),
            cost_estimate=pl.CostEstimate(flops=SEQ * weight_bytes, bytes_accessed=weight_bytes, transcendentals=0),
        )(x_local, ln1_gain, w_qkv, w_out, ln2_gain, w_up, w_down)

    return jax.shard_map(layer_stack, mesh=mesh, in_specs=(P('dp', 'tp', None), P(), P(None, None, 'tp', None), P(None, 'tp', None, None), P(), P(None, None, 'tp'), P(None, 'tp', None)), out_specs=P('dp', 'tp', None), check_vma=False)
```

```python
import functools

import jax
import jax.numpy as jnp
from jax import lax
from jax.experimental import pallas as pl
from jax.experimental.pallas import tpu as pltpu
from jax.sharding import PartitionSpec as P

LN_EPS = 1.0e-5
NEG_BIG = -1.0e30
MESH = pl.DeviceIdType.MESH

TP = 4
SEQ = 128
ROWS = SEQ // TP
D = 5120
C = 1280
NC = D // C
HEADS = 10
HD = 128
SLOTS = 17
TILES = 48
LAYERS = 2
NW = 256


def stack_kernel(x_hbm, g1_hbm, wqkv_hbm, wout_hbm, g2_hbm, wup_hbm, wdown_hbm, y_hbm,
                 ring, x_all, a_buf, stat, q_stat, mean_b, scale_b, hid, acc, p_snd, p_rcv, q_snd, q_rcv, g1_ref, g2_ref,
                 ring_sem, x_sem, g_sem, ag_s, ag_r, st_s, st_r, p_s, p_r, q_s, q_r):
    me = lax.axis_index('tp')
    partner = me + 1 - 2 * lax.rem(me, 2)
    cross = lax.rem(me + 2, TP)
    diag = lax.rem(partner + 2, TP)

    def slot_of(layer, i):
        return lax.rem(TILES * layer + i, SLOTS)

    def tile(w, layer, row, col, slot):
        rows = pl.ds(pl.multiple_of(row * C, C), C)
        cols = pl.ds(pl.multiple_of(col * C, C), C)
        return pltpu.make_async_copy(w.at[layer, rows, cols], ring.at[slot], ring_sem.at[slot])

    def start_qkv(layer, i):
        j, s = i // 3, i % 3
        slot = slot_of(layer, i)
        rows = pl.ds(j * C, C)
        pieces, col = [], 0
        for head in range(HEADS):
            lo, hi = head * 3 * HD, (head + 1) * 3 * HD
            a, b = max(lo, s * C), min(hi, (s + 1) * C)
            if a < b:
                pieces.append((head, a - lo, b - a, a - s * C))
        for head, src, width, dst in pieces:
            pltpu.make_async_copy(wqkv_hbm.at[layer, head, rows, pl.ds(src, width)],
                                  ring.at[slot, :, pl.ds(dst, width)], ring_sem.at[slot]).start(priority=1)

    def start_attention_tile(layer, i):
        if i < 12:
            start_qkv(layer, i)
        else:
            tile(wout_hbm, layer, 0, i - 12, slot_of(layer, i)).start(priority=1)

    def start_up(layer, i):
        tile(wup_hbm, layer, i // NC, lax.rem(i, NC), slot_of(layer, 16 + i)).start(priority=1)

    def start_down(layer, i):
        tile(wdown_hbm, layer, lax.rem(i, NC), i // NC, slot_of(layer, 32 + i)).start(priority=1)

    def wait_tile(layer, i):
        tile(wup_hbm, 0, 0, 0, slot_of(layer, i)).wait()

    def refill(layer, i):
        t = i + SLOTS
        if not isinstance(t, int):
            raise TypeError('static tile')
        if t < 32:
            start_up(layer, t - 16)
        elif t < TILES:
            start_down(layer, t - 32)
        else:
            @pl.when(layer < LAYERS - 1)
            def _():
                if t < TILES + 16:
                    start_attention_tile(layer + 1, t - TILES)
                else:
                    start_up(layer + 1, t - TILES - 16)

    def block(jobs):
        for pairs, dst, add, finish in jobs:
            for n in range(C // NW):
                cols = pl.ds(n * NW, NW)
                part = None
                for lhs, slot in pairs:
                    term = jnp.dot(lhs(), ring[slot, :, cols], preferred_element_type=jnp.float32)
                    part = term if part is None else part + term
                if add:
                    part = part + acc[dst, :, :, cols].reshape(SEQ, NW)
                if finish is None:
                    acc[dst, :, :, cols] = part.reshape(TP, ROWS, NW)
                else:
                    finish(part, dst, cols)

    def remote(src, dst, send_sem, recv_sem, peer):
        return pltpu.make_async_remote_copy(src_ref=src, dst_ref=dst, send_sem=send_sem, recv_sem=recv_sem,
                                            device_id={'tp': peer}, device_id_type=MESH)

    def ag_copy(j, kind):
        source, peer = ((me, partner), (me, cross), (cross, partner))[kind]
        return remote(x_all.at[j, source], x_all.at[j, source], ag_s.at[kind, j], ag_r.at[kind, j], peer)

    def ag_wait(j, kind):
        source = (partner, cross, diag)[kind]
        remote(x_all.at[j, source], x_all.at[j, source], ag_s.at[kind, j], ag_r.at[kind, j], partner).wait_recv()

    def ag_send(j):
        ag_copy(j, 1).start()
        ag_copy(j, 0).start()

    def forward(j):
        ag_wait(j, 1)
        ag_copy(j, 2).start()

    def stat_copy(k):
        return remote(stat.at[me], stat.at[me], st_s.at[k], st_r.at[k], (partner, cross, diag)[k])

    def quarter_stats(j):
        x = x_all[j, me].astype(jnp.float32)
        mean = jnp.sum(x, axis=-1, keepdims=True) / C
        centered = x - mean
        q_stat[j, 0] = jnp.broadcast_to(mean, (ROWS, HD))
        q_stat[j, 1] = jnp.broadcast_to(jnp.sum(centered * centered, axis=-1, keepdims=True), (ROWS, HD))

    def stats_send():
        mean = (q_stat[0, 0] + q_stat[1, 0] + q_stat[2, 0] + q_stat[3, 0]) / NC
        square = jnp.zeros((ROWS, HD), jnp.float32)
        for j in range(NC):
            shift = q_stat[j, 0] - mean
            square += q_stat[j, 1] + C * (shift * shift)
        scale = lax.rsqrt(square / D + LN_EPS)
        lanes = lax.broadcasted_iota(jnp.int32, (8, HD), 1)
        packed = jnp.zeros((8, HD), jnp.float32)
        for i in range(ROWS // 8):
            packed = jnp.where(lanes == i, mean[8 * i:8 * i + 8], packed)
            packed = jnp.where(lanes == 4 + i, scale[8 * i:8 * i + 8], packed)
        stat[me] = packed
        for k in (1, 2, 0):
            stat_copy(k).start()

    def stats_wait():
        for k, source in enumerate((partner, cross, diag)):
            remote(stat.at[source], stat.at[source], st_s.at[k], st_r.at[k], partner).wait_recv()
        for source in range(TP):
            packed = stat[source]
            for i in range(ROWS // 8):
                rows = pl.ds(source * ROWS + 8 * i, 8)
                mean_b[rows] = jnp.broadcast_to(packed[:, i:i + 1], (8, HD))
                scale_b[rows] = jnp.broadcast_to(packed[:, 4 + i:5 + i], (8, HD))

    def ag_drain():
        for j in range(NC):
            for kind in range(3):
                ag_copy(j, kind).wait_send()
        for k in range(3):
            stat_copy(k).wait_send()

    def normalize(j, g_ref, layer):
        mean, scale = mean_b[...], scale_b[...]
        for k in range(C // HD):
            cols = pl.ds(k * HD, HD)
            gains = g_ref[:, pl.ds(pl.multiple_of(j * C + k * HD, HD), HD)]
            gain = jnp.where(layer == 0, gains[0:1], gains[1:2])
            x = x_all[j, :, :, cols].reshape(SEQ, HD).astype(jnp.float32)
            a_buf[:, cols] = ((x - mean) * scale * gain).astype(jnp.bfloat16)

    def when(cond, body):
        if isinstance(cond, bool):
            if cond:
                body()
        else:
            pl.when(cond)(body)

    def rs_p(q):
        return remote(p_snd.at[lax.rem(q, 2)], p_rcv.at[q], p_s.at[q], p_r.at[q], partner)

    def rs_q(q):
        return remote(q_snd.at[lax.rem(q, 2)], q_rcv.at[q], q_s.at[q], q_r.at[q], cross)

    def rs_a(q):
        when(q >= 2, lambda: rs_p(q - 2).wait_send())
        p_snd[lax.rem(q, 2), 0] = acc[q, partner].astype(jnp.bfloat16)
        p_snd[lax.rem(q, 2), 1] = acc[q, diag].astype(jnp.bfloat16)
        rs_p(q).start()

    def rs_b(q):
        rs_p(q).wait_recv()
        when(q >= 2, lambda: rs_q(q - 2).wait_send())
        q_snd[lax.rem(q, 2)] = (acc[q, cross] + p_rcv[q, 1].astype(jnp.float32)).astype(jnp.bfloat16)
        rs_q(q).start()

    def rs_c(q):
        rs_q(q).wait_recv()
        total = acc[q, me] + p_rcv[q, 0].astype(jnp.float32) + q_rcv[q].astype(jnp.float32)
        x_all[q, me] = (x_all[q, me].astype(jnp.float32) + total).astype(jnp.bfloat16)
        quarter_stats(q)

    def rs_drain():
        for q in range(2, NC):
            rs_p(q).wait_send()
            rs_q(q).wait_send()

    def attention():
        keys = lax.broadcasted_iota(jnp.int32, (SEQ, SEQ), 0)
        queries = lax.broadcasted_iota(jnp.int32, (SEQ, SEQ), 1)
        causal = queries >= keys

        def part(block):
            third, col = block * HD // C, block * HD % C
            return acc[third, :, :, pl.ds(col, HD)].reshape(SEQ, HD).astype(jnp.bfloat16)

        for head in range(HEADS):
            query, key = part(3 * head), part(3 * head + 1)
            scores = lax.dot_general(key, query, (((1,), (1,)), ((), ())), preferred_element_type=jnp.float32)
            scores = jnp.where(causal, scores * HD ** -0.5, NEG_BIG)
            acc[3, :, :, pl.ds(head * HD, HD)] = scores.reshape(TP, ROWS, HD)
        for head in range(HEADS):
            scores = acc[3, :, :, pl.ds(head * HD, HD)].reshape(SEQ, SEQ)
            probs = jnp.exp(scores - jnp.max(scores, axis=0, keepdims=True))
            hid[0, :, pl.ds(head * HD, HD)] = (probs / jnp.sum(probs, axis=0, keepdims=True)).astype(jnp.bfloat16)
        for head in range(HEADS):
            out = lax.dot_general(hid[0, :, pl.ds(head * HD, HD)], part(3 * head + 2), (((0,), (0,)), ((), ())),
                                  preferred_element_type=jnp.float32)
            a_buf[:, pl.ds(head * HD, HD)] = out.astype(jnp.bfloat16)

    x_copies = [pltpu.make_async_copy(x_hbm.at[0, :, pl.ds(j * C, C)], x_all.at[j, me], x_sem.at[j]) for j in range(NC)]
    g_copies = [pltpu.make_async_copy(g1_hbm, g1_ref, g_sem.at[0]), pltpu.make_async_copy(g2_hbm, g2_ref, g_sem.at[1])]
    for copy in x_copies + g_copies:
        copy.start()
    for i in range(16):
        start_attention_tile(0, i)
    for i in range(SLOTS - 16):
        start_up(0, i)
    barrier = pltpu.get_barrier_semaphore()
    for peer in (partner, cross, diag):
        pl.semaphore_signal(barrier, inc=1, device_id={'tp': peer}, device_id_type=MESH)
    pl.semaphore_wait(barrier, 3)
    for copy in x_copies + g_copies:
        copy.wait()

    def loop(lo, hi, body):
        lax.fori_loop(lo, hi, lambda i, carry: (body(i), carry)[1], 0)

    def chunks(chunk):
        stats_wait()

        def one(j, first, last):
            ag_wait(j, 0)
            ag_wait(j, 2)
            chunk(j, first, last)

        one(0, True, False)
        forward(2)

        def middle(j):
            one(j, False, False)

            @pl.when(j == 1)
            def _():
                forward(3)

        loop(1, NC - 1, middle)
        one(NC - 1, False, True)

    def layer_body(layer):
        more = layer < LAYERS - 1

        def qkv_chunk(j, first, last):
            for t in range(3):
                wait_tile(layer, 3 * j + t)
            normalize(j, g1_ref, layer)
            block([([(lambda: a_buf[...], slot_of(layer, 3 * j + t))], t, not first, None) for t in range(3)])
            for t in range(3):
                start_up(layer, 3 * j + t + SLOTS - 16)

        chunks(qkv_chunk)
        attention()
        ag_drain()

        def out_tiles(quarters):
            for q in quarters:
                wait_tile(layer, 12 + q)
            block([([(lambda: a_buf[...], slot_of(layer, 12 + q))], q, False, None) for q in quarters])
            for q in quarters:
                rs_a(q)
            for q in quarters:
                refill(layer, 12 + q)

        out_tiles((0,))
        out_tiles((1, 2))
        rs_b(0)
        out_tiles((3,))
        loop(1, NC, rs_b)
        for q in range(NC):
            rs_c(q)
            if q < 2:
                ag_send(q)
        stats_send()
        ag_send(2)
        ag_send(3)
        forward(0)
        forward(1)
        rs_drain()

        def gelu_out(part, q, cols):
            hid[q, :, cols] = jax.nn.gelu(part, approximate=True).astype(jnp.bfloat16)

        def up_chunk(j, first, last):
            for group in ((0,), (1,), (2, 3)) if first else ((0, 1, 2, 3),):
                for q in group:
                    wait_tile(layer, 16 + NC * j + q)
                if group[0] == 0:
                    normalize(j, g2_ref, layer)
                block([([(lambda: a_buf[...], slot_of(layer, 16 + NC * j + q))], q, not first,
                        gelu_out if last else None) for q in group])
                for q in group:
                    if last:
                        refill(layer, 16 + NC * j + q)
                    else:
                        start_down(layer, NC * j + q + SLOTS - 16)

        chunks(up_chunk)
        ag_drain()

        def down_tiles(q, chunk_ids, add):
            for j in chunk_ids:
                wait_tile(layer, 32 + NC * q + j)
            block([([(functools.partial(lambda j: hid[j], j), slot_of(layer, 32 + NC * q + j)) for j in chunk_ids],
                    q, add, None)])

            for k in range(NC):
                if isinstance(q, int):
                    if q == k:
                        for j in chunk_ids:
                            refill(layer, 32 + NC * k + j)
                else:
                    @pl.when(q == k)
                    def _():
                        for j in chunk_ids:
                            refill(layer, 32 + NC * k + j)

        def down_quarter(q):
            down_tiles(q, (0, 1, 2, 3), False)
            rs_a(q)

            @pl.when(q >= 1)
            def _():
                rs_b(q - 1)

        loop(0, NC - 1, down_quarter)
        down_tiles(3, (0, 1), False)
        rs_b(2)
        rs_c(0)

        @pl.when(more)
        def _():
            ag_send(0)

        down_tiles(3, (2,), True)
        down_tiles(3, (3,), True)
        rs_a(3)
        rs_c(1)
        rs_b(3)

        @pl.when(more)
        def _():
            ag_send(1)

        rs_c(2)

        @pl.when(more)
        def _():
            forward(0)

        rs_c(3)

        @pl.when(more)
        def _():
            stats_send()
            ag_send(2)
            ag_send(3)
            forward(1)

        rs_drain()

    ag_send(0)
    for j in range(NC):
        quarter_stats(j)
    stats_send()
    for j in range(1, NC):
        ag_send(j)
    forward(0)
    forward(1)
    loop(0, LAYERS, layer_body)
    y_copies = [pltpu.make_async_copy(x_all.at[j, me], y_hbm.at[0, :, pl.ds(j * C, C)], x_sem.at[j]) for j in range(NC)]
    for copy in y_copies:
        copy.start()
    for copy in y_copies:
        copy.wait()


def solution(mesh):
    def layer_stack(x_local, ln1_gain, w_qkv, w_out, ln2_gain, w_up, w_down):
        w_qkv = jnp.transpose(w_qkv, (0, 2, 1, 3))
        w_out = w_out.reshape(LAYERS, HEADS * HD, D)
        hbm = pl.BlockSpec(memory_space=pl.ANY)
        weight_bytes = 2 * LAYERS * (3 * C * D + C * D + 2 * D * D)
        return pl.pallas_call(
            stack_kernel,
            out_shape=jax.ShapeDtypeStruct(x_local.shape, jnp.bfloat16),
            in_specs=[hbm] * 7,
            out_specs=hbm,
            scratch_shapes=[
                pltpu.VMEM((SLOTS, C, C), jnp.bfloat16),
                pltpu.VMEM((NC, TP, ROWS, C), jnp.bfloat16),
                pltpu.VMEM((SEQ, C), jnp.bfloat16),
                pltpu.VMEM((TP, 8, HD), jnp.float32),
                pltpu.VMEM((NC, 2, ROWS, HD), jnp.float32),
                pltpu.VMEM((SEQ, HD), jnp.float32),
                pltpu.VMEM((SEQ, HD), jnp.float32),
                pltpu.VMEM((NC, SEQ, C), jnp.bfloat16),
                pltpu.VMEM((NC, TP, ROWS, C), jnp.float32),
                pltpu.VMEM((2, 2, ROWS, C), jnp.bfloat16),
                pltpu.VMEM((NC, 2, ROWS, C), jnp.bfloat16),
                pltpu.VMEM((2, ROWS, C), jnp.bfloat16),
                pltpu.VMEM((NC, ROWS, C), jnp.bfloat16),
                pltpu.VMEM((LAYERS, D), jnp.float32),
                pltpu.VMEM((LAYERS, D), jnp.float32),
                pltpu.SemaphoreType.DMA((SLOTS,)),
                pltpu.SemaphoreType.DMA((NC,)),
                pltpu.SemaphoreType.DMA((2,)),
                pltpu.SemaphoreType.DMA((3, NC)),
                pltpu.SemaphoreType.DMA((3, NC)),
                pltpu.SemaphoreType.DMA((3,)),
                pltpu.SemaphoreType.DMA((3,)),
                pltpu.SemaphoreType.DMA((NC,)),
                pltpu.SemaphoreType.DMA((NC,)),
                pltpu.SemaphoreType.DMA((NC,)),
                pltpu.SemaphoreType.DMA((NC,)),
            ],
            compiler_params=pltpu.CompilerParams(collective_id=0, has_side_effects=True, vmem_limit_bytes=67_043_328),
            cost_estimate=pl.CostEstimate(flops=SEQ * weight_bytes, bytes_accessed=weight_bytes, transcendentals=0),
        )(x_local, ln1_gain, w_qkv, w_out, ln2_gain, w_up, w_down)

    return jax.shard_map(layer_stack, mesh=mesh, in_specs=(P('dp', 'tp', None), P(), P(None, None, 'tp', None), P(None, 'tp', None, None), P(), P(None, None, 'tp'), P(None, 'tp', None)), out_specs=P('dp', 'tp', None), check_vma=False)
```

```python
import functools

import jax
import jax.numpy as jnp
from jax import lax
from jax.experimental import pallas as pl
from jax.experimental.pallas import tpu as pltpu
from jax.sharding import PartitionSpec as P

LN_EPS = 1.0e-5
NEG_BIG = -1.0e30
MESH = pl.DeviceIdType.MESH

TP = 4
SEQ = 128
ROWS = SEQ // TP
D = 5120
C = 1280
NC = D // C
HEADS = 10
HD = 128
SLOTS = 17
TILES = 48
LAYERS = 2
NW = 256


def stack_kernel(x_hbm, g1_hbm, wqkv_hbm, wout_hbm, g2_hbm, wup_hbm, wdown_hbm, y_hbm,
                 ring, x_all, a_buf, stat, q_stat, mean_b, scale_b, hid, acc, p_snd, p_rcv, q_snd, q_rcv, g1_ref, g2_ref,
                 ring_sem, x_sem, g_sem, ag_s, ag_r, st_s, st_r, p_s, p_r, q_s, q_r):
    me = lax.axis_index('tp')
    partner = me + 1 - 2 * lax.rem(me, 2)
    cross = lax.rem(me + 2, TP)
    diag = lax.rem(partner + 2, TP)

    def slot_of(layer, i):
        return lax.rem(TILES * layer + i, SLOTS)

    def tile(w, layer, row, col, slot):
        rows = pl.ds(pl.multiple_of(row * C, C), C)
        cols = pl.ds(pl.multiple_of(col * C, C), C)
        return pltpu.make_async_copy(w.at[layer, rows, cols], ring.at[slot], ring_sem.at[slot])

    def start_qkv(layer, i):
        j, s = i // 3, i % 3
        slot = slot_of(layer, i)
        rows = pl.ds(j * C, C)
        pieces, col = [], 0
        for head in range(HEADS):
            lo, hi = head * 3 * HD, (head + 1) * 3 * HD
            a, b = max(lo, s * C), min(hi, (s + 1) * C)
            if a < b:
                pieces.append((head, a - lo, b - a, a - s * C))
        for head, src, width, dst in pieces:
            pltpu.make_async_copy(wqkv_hbm.at[layer, head, rows, pl.ds(src, width)],
                                  ring.at[slot, :, pl.ds(dst, width)], ring_sem.at[slot]).start(priority=1)

    def start_attention_tile(layer, i):
        if i < 12:
            start_qkv(layer, i)
        else:
            tile(wout_hbm, layer, 0, i - 12, slot_of(layer, i)).start(priority=1)

    def start_up(layer, i):
        tile(wup_hbm, layer, i // NC, lax.rem(i, NC), slot_of(layer, 16 + i)).start(priority=1)

    def start_down(layer, i):
        tile(wdown_hbm, layer, lax.rem(i, NC), i // NC, slot_of(layer, 32 + i)).start(priority=1)

    def wait_tile(layer, i):
        tile(wup_hbm, 0, 0, 0, slot_of(layer, i)).wait()

    def refill(layer, i):
        t = i + SLOTS
        if not isinstance(t, int):
            raise TypeError('static tile')
        if t < 32:
            start_up(layer, t - 16)
        elif t < TILES:
            start_down(layer, t - 32)
        else:
            @pl.when(layer < LAYERS - 1)
            def _():
                if t < TILES + 16:
                    start_attention_tile(layer + 1, t - TILES)
                else:
                    start_up(layer + 1, t - TILES - 16)

    def block(jobs):
        for pairs, dst, add, finish in jobs:
            for n in range(C // NW):
                cols = pl.ds(n * NW, NW)
                part = None
                for lhs, slot in pairs:
                    term = jnp.dot(lhs(), ring[slot, :, cols], preferred_element_type=jnp.float32)
                    part = term if part is None else part + term
                if add:
                    part = part + acc[dst, :, :, cols].reshape(SEQ, NW)
                if finish is None:
                    acc[dst, :, :, cols] = part.reshape(TP, ROWS, NW)
                else:
                    finish(part, dst, cols)

    def remote(src, dst, send_sem, recv_sem, peer):
        return pltpu.make_async_remote_copy(src_ref=src, dst_ref=dst, send_sem=send_sem, recv_sem=recv_sem,
                                            device_id={'tp': peer}, device_id_type=MESH)

    def ag_copy(j, kind):
        source, peer = ((me, partner), (me, cross), (cross, partner))[kind]
        return remote(x_all.at[j, source], x_all.at[j, source], ag_s.at[kind, j], ag_r.at[kind, j], peer)

    def ag_wait(j, kind):
        source = (partner, cross, diag)[kind]
        remote(x_all.at[j, source], x_all.at[j, source], ag_s.at[kind, j], ag_r.at[kind, j], partner).wait_recv()

    def ag_send(j):
        ag_copy(j, 1).start()
        ag_copy(j, 0).start()

    def forward(j):
        ag_wait(j, 1)
        ag_copy(j, 2).start()

    def stat_copy(k):
        return remote(stat.at[me], stat.at[me], st_s.at[k], st_r.at[k], (partner, cross, diag)[k])

    def quarter_stats(j):
        x = x_all[j, me].astype(jnp.float32)
        mean = jnp.sum(x, axis=-1, keepdims=True) / C
        centered = x - mean
        q_stat[j, 0] = jnp.broadcast_to(mean, (ROWS, HD))
        q_stat[j, 1] = jnp.broadcast_to(jnp.sum(centered * centered, axis=-1, keepdims=True), (ROWS, HD))

    def stats_send():
        mean = (q_stat[0, 0] + q_stat[1, 0] + q_stat[2, 0] + q_stat[3, 0]) / NC
        square = jnp.zeros((ROWS, HD), jnp.float32)
        for j in range(NC):
            shift = q_stat[j, 0] - mean
            square += q_stat[j, 1] + C * (shift * shift)
        scale = lax.rsqrt(square / D + LN_EPS)
        lanes = lax.broadcasted_iota(jnp.int32, (8, HD), 1)
        packed = jnp.zeros((8, HD), jnp.float32)
        for i in range(ROWS // 8):
            packed = jnp.where(lanes == i, mean[8 * i:8 * i + 8], packed)
            packed = jnp.where(lanes == 4 + i, scale[8 * i:8 * i + 8], packed)
        stat[me] = packed
        for k in (1, 2, 0):
            stat_copy(k).start()

    def stats_wait():
        for k, source in enumerate((partner, cross, diag)):
            remote(stat.at[source], stat.at[source], st_s.at[k], st_r.at[k], partner).wait_recv()
        for source in range(TP):
            packed = stat[source]
            for i in range(ROWS // 8):
                rows = pl.ds(source * ROWS + 8 * i, 8)
                mean_b[rows] = jnp.broadcast_to(packed[:, i:i + 1], (8, HD))
                scale_b[rows] = jnp.broadcast_to(packed[:, 4 + i:5 + i], (8, HD))

    def ag_drain():
        for j in range(NC):
            for kind in range(3):
                ag_copy(j, kind).wait_send()
        for k in range(3):
            stat_copy(k).wait_send()

    def normalize(j, g_ref, layer):
        mean, scale = mean_b[...], scale_b[...]
        for k in range(C // HD):
            cols = pl.ds(k * HD, HD)
            gains = g_ref[:, pl.ds(pl.multiple_of(j * C + k * HD, HD), HD)]
            gain = jnp.where(layer == 0, gains[0:1], gains[1:2])
            x = x_all[j, :, :, cols].reshape(SEQ, HD).astype(jnp.float32)
            a_buf[:, cols] = ((x - mean) * scale * gain).astype(jnp.bfloat16)

    def when(cond, body):
        if isinstance(cond, bool):
            if cond:
                body()
        else:
            pl.when(cond)(body)

    def rs_p(q):
        return remote(p_snd.at[lax.rem(q, 2)], p_rcv.at[q], p_s.at[q], p_r.at[q], partner)

    def rs_q(q):
        return remote(q_snd.at[lax.rem(q, 2)], q_rcv.at[q], q_s.at[q], q_r.at[q], cross)

    def rs_a(q):
        when(q >= 2, lambda: rs_p(q - 2).wait_send())
        p_snd[lax.rem(q, 2), 0] = acc[q, partner].astype(jnp.bfloat16)
        p_snd[lax.rem(q, 2), 1] = acc[q, diag].astype(jnp.bfloat16)
        rs_p(q).start()

    def rs_b(q):
        rs_p(q).wait_recv()
        when(q >= 2, lambda: rs_q(q - 2).wait_send())
        q_snd[lax.rem(q, 2)] = (acc[q, cross] + p_rcv[q, 1].astype(jnp.float32)).astype(jnp.bfloat16)
        rs_q(q).start()

    def rs_c(q):
        rs_q(q).wait_recv()
        total = acc[q, me] + p_rcv[q, 0].astype(jnp.float32) + q_rcv[q].astype(jnp.float32)
        x_all[q, me] = (x_all[q, me].astype(jnp.float32) + total).astype(jnp.bfloat16)
        quarter_stats(q)

    def rs_drain():
        for q in range(2, NC):
            rs_p(q).wait_send()
            rs_q(q).wait_send()

    def attention():
        keys = lax.broadcasted_iota(jnp.int32, (SEQ, SEQ), 0)
        queries = lax.broadcasted_iota(jnp.int32, (SEQ, SEQ), 1)
        causal = queries >= keys

        def part(block):
            third, col = block * HD // C, block * HD % C
            return acc[third, :, :, pl.ds(col, HD)].reshape(SEQ, HD).astype(jnp.bfloat16)

        for head in range(HEADS):
            query, key = part(3 * head), part(3 * head + 1)
            scores = lax.dot_general(key, query, (((1,), (1,)), ((), ())), preferred_element_type=jnp.float32)
            scores = jnp.where(causal, scores * HD ** -0.5, NEG_BIG)
            acc[3, :, :, pl.ds(head * HD, HD)] = scores.reshape(TP, ROWS, HD)
        for head in range(HEADS):
            scores = acc[3, :, :, pl.ds(head * HD, HD)].reshape(SEQ, SEQ)
            probs = jnp.exp(scores - jnp.max(scores, axis=0, keepdims=True))
            hid[0, :, pl.ds(head * HD, HD)] = (probs / jnp.sum(probs, axis=0, keepdims=True)).astype(jnp.bfloat16)
        for head in range(HEADS):
            out = lax.dot_general(hid[0, :, pl.ds(head * HD, HD)], part(3 * head + 2), (((0,), (0,)), ((), ())),
                                  preferred_element_type=jnp.float32)
            a_buf[:, pl.ds(head * HD, HD)] = out.astype(jnp.bfloat16)

    x_copies = [pltpu.make_async_copy(x_hbm.at[0, :, pl.ds(j * C, C)], x_all.at[j, me], x_sem.at[j]) for j in range(NC)]
    g_copies = [pltpu.make_async_copy(g1_hbm, g1_ref, g_sem.at[0]), pltpu.make_async_copy(g2_hbm, g2_ref, g_sem.at[1])]
    for copy in x_copies + g_copies:
        copy.start()
    for i in range(16):
        start_attention_tile(0, i)
    for i in range(SLOTS - 16):
        start_up(0, i)
    barrier = pltpu.get_barrier_semaphore()
    for peer in (partner, cross, diag):
        pl.semaphore_signal(barrier, inc=1, device_id={'tp': peer}, device_id_type=MESH)
    pl.semaphore_wait(barrier, 3)
    for copy in x_copies + g_copies:
        copy.wait()

    def loop(lo, hi, body):
        lax.fori_loop(lo, hi, lambda i, carry: (body(i), carry)[1], 0)

    def chunks(chunk):
        stats_wait()

        def one(j, first, last):
            ag_wait(j, 0)
            ag_wait(j, 2)
            chunk(j, first, last)

        one(0, True, False)
        forward(2)

        def middle(j):
            one(j, False, False)

            @pl.when(j == 1)
            def _():
                forward(3)

        loop(1, NC - 1, middle)
        one(NC - 1, False, True)

    def layer_body(layer):
        more = layer < LAYERS - 1

        def qkv_chunk(j, first, last):
            for t in range(3):
                wait_tile(layer, 3 * j + t)
            normalize(j, g1_ref, layer)
            block([([(lambda: a_buf[...], slot_of(layer, 3 * j + t))], t, not first, None) for t in range(3)])
            for t in range(3):
                start_up(layer, 3 * j + t + SLOTS - 16)

        chunks(qkv_chunk)
        wait_tile(layer, 12)
        attention()

        def out_tiles(quarters):
            for q in quarters:
                if q > 0:
                    wait_tile(layer, 12 + q)
            block([([(lambda: a_buf[...], slot_of(layer, 12 + q))], q, False, None) for q in quarters])
            for q in quarters:
                rs_a(q)
            for q in quarters:
                refill(layer, 12 + q)

        out_tiles((0,))
        out_tiles((1, 2))
        ag_drain()
        rs_b(0)
        out_tiles((3,))
        loop(1, NC, rs_b)
        for q in range(NC):
            rs_c(q)
            if q < 2:
                ag_send(q)
        stats_send()
        ag_send(2)
        ag_send(3)
        forward(0)
        forward(1)
        rs_drain()

        def gelu_out(part, q, cols):
            hid[q, :, cols] = jax.nn.gelu(part, approximate=True).astype(jnp.bfloat16)

        def up_chunk(j, first, last):
            for group in ((0,), (1,), (2, 3)) if first else ((0, 1, 2, 3),):
                for q in group:
                    wait_tile(layer, 16 + NC * j + q)
                if group[0] == 0:
                    normalize(j, g2_ref, layer)
                block([([(lambda: a_buf[...], slot_of(layer, 16 + NC * j + q))], q, not first,
                        gelu_out if last else None) for q in group])
                for q in group:
                    if last:
                        refill(layer, 16 + NC * j + q)
                    else:
                        start_down(layer, NC * j + q + SLOTS - 16)

        chunks(up_chunk)

        def down_tiles(q, chunk_ids, add):
            for j in chunk_ids:
                wait_tile(layer, 32 + NC * q + j)
            block([([(functools.partial(lambda j: hid[j], j), slot_of(layer, 32 + NC * q + j)) for j in chunk_ids],
                    q, add, None)])

            for k in range(NC):
                if isinstance(q, int):
                    if q == k:
                        for j in chunk_ids:
                            refill(layer, 32 + NC * k + j)
                else:
                    @pl.when(q == k)
                    def _():
                        for j in chunk_ids:
                            refill(layer, 32 + NC * k + j)

        def down_quarter(q):
            down_tiles(q, (0, 1, 2, 3), False)
            rs_a(q)

            @pl.when(q == 0)
            def _():
                ag_drain()

            @pl.when(q >= 1)
            def _():
                rs_b(q - 1)

        loop(0, NC - 1, down_quarter)
        down_tiles(3, (0, 1), False)
        rs_b(2)
        rs_c(0)

        @pl.when(more)
        def _():
            ag_send(0)

        down_tiles(3, (2,), True)
        down_tiles(3, (3,), True)
        rs_a(3)
        rs_c(1)
        rs_b(3)

        @pl.when(more)
        def _():
            ag_send(1)

        rs_c(2)

        @pl.when(more)
        def _():
            forward(0)

        rs_c(3)

        @pl.when(more)
        def _():
            stats_send()
            ag_send(2)
            ag_send(3)
            forward(1)

        rs_drain()

    ag_send(0)
    for j in range(NC):
        quarter_stats(j)
    stats_send()
    for j in range(1, NC):
        ag_send(j)
    forward(0)
    forward(1)
    loop(0, LAYERS, layer_body)
    y_copies = [pltpu.make_async_copy(x_all.at[j, me], y_hbm.at[0, :, pl.ds(j * C, C)], x_sem.at[j]) for j in range(NC)]
    for copy in y_copies:
        copy.start()
    for copy in y_copies:
        copy.wait()


def solution(mesh):
    def layer_stack(x_local, ln1_gain, w_qkv, w_out, ln2_gain, w_up, w_down):
        w_qkv = jnp.transpose(w_qkv, (0, 2, 1, 3))
        w_out = w_out.reshape(LAYERS, HEADS * HD, D)
        hbm = pl.BlockSpec(memory_space=pl.ANY)
        weight_bytes = 2 * LAYERS * (3 * C * D + C * D + 2 * D * D)
        return pl.pallas_call(
            stack_kernel,
            out_shape=jax.ShapeDtypeStruct(x_local.shape, jnp.bfloat16),
            in_specs=[hbm] * 7,
            out_specs=hbm,
            scratch_shapes=[
                pltpu.VMEM((SLOTS, C, C), jnp.bfloat16),
                pltpu.VMEM((NC, TP, ROWS, C), jnp.bfloat16),
                pltpu.VMEM((SEQ, C), jnp.bfloat16),
                pltpu.VMEM((TP, 8, HD), jnp.float32),
                pltpu.VMEM((NC, 2, ROWS, HD), jnp.float32),
                pltpu.VMEM((SEQ, HD), jnp.float32),
                pltpu.VMEM((SEQ, HD), jnp.float32),
                pltpu.VMEM((NC, SEQ, C), jnp.bfloat16),
                pltpu.VMEM((NC, TP, ROWS, C), jnp.float32),
                pltpu.VMEM((2, 2, ROWS, C), jnp.bfloat16),
                pltpu.VMEM((NC, 2, ROWS, C), jnp.bfloat16),
                pltpu.VMEM((2, ROWS, C), jnp.bfloat16),
                pltpu.VMEM((NC, ROWS, C), jnp.bfloat16),
                pltpu.VMEM((LAYERS, D), jnp.float32),
                pltpu.VMEM((LAYERS, D), jnp.float32),
                pltpu.SemaphoreType.DMA((SLOTS,)),
                pltpu.SemaphoreType.DMA((NC,)),
                pltpu.SemaphoreType.DMA((2,)),
                pltpu.SemaphoreType.DMA((3, NC)),
                pltpu.SemaphoreType.DMA((3, NC)),
                pltpu.SemaphoreType.DMA((3,)),
                pltpu.SemaphoreType.DMA((3,)),
                pltpu.SemaphoreType.DMA((NC,)),
                pltpu.SemaphoreType.DMA((NC,)),
                pltpu.SemaphoreType.DMA((NC,)),
                pltpu.SemaphoreType.DMA((NC,)),
            ],
            compiler_params=pltpu.CompilerParams(collective_id=0, has_side_effects=True, vmem_limit_bytes=67_043_328),
            cost_estimate=pl.CostEstimate(flops=SEQ * weight_bytes, bytes_accessed=weight_bytes, transcendentals=0),
        )(x_local, ln1_gain, w_qkv, w_out, ln2_gain, w_up, w_down)

    return jax.shard_map(layer_stack, mesh=mesh, in_specs=(P('dp', 'tp', None), P(), P(None, None, 'tp', None), P(None, 'tp', None, None), P(), P(None, None, 'tp'), P(None, 'tp', None)), out_specs=P('dp', 'tp', None), check_vma=False)
```
